64 devices in a mesh: rep: 4 (over x, y), dp: 16 (over z, core).
Axes of the slice: x: 2, y: 2, z: 8, core: 2. Of those that a mesh axis runs over, the one named last changes fastest.
The devices are a block of a 4x4x8 slice.
Arguments:
- x: bfloat16 [64, 2048, 512], P(('rep', 'dp')), parts along dimension 0
- dy: bfloat16 [64, 2048, 512], P(('rep', 'dp')), parts along dimension 0
- w_gate: bfloat16 [2, 512, 2560], P(None, 'dp')
- w_up: bfloat16 [2, 512, 2560], P(None, 'dp')
- w_down: bfloat16 [2, 2560, 512], P(None, 'dp')
Outputs:
- output 1: bfloat16 [64, 2048, 512], P(('rep', 'dp')), parts along dimension 0
- output 2: bfloat16 [8, 512, 2560], P('rep', 'dp'), parts along dimension 0
- output 3: bfloat16 [8, 512, 2560], P('rep', 'dp'), parts along dimension 0
- output 4: bfloat16 [8, 2560, 512], P('rep', 'dp'), parts along dimension 0
There are 4 independent parts. The reference program is written for one: setup_inputs(seed, part) draws one part's arguments, and reference() takes and returns one part's arrays. A program takes and returns all parts, laid end to end along the dimension named above; an argument that names none is the same for every part.
All inputs are finite; a program needn't handle non-finite values.
Results may differ from the reference program's by a relative error of at most 0.018.
Values are sent between devices in bfloat16 or wider.
A program may use at most 768 MiB of HBM per device.

```python
import jax
import jax.numpy as jnp
from jax import lax

SEQUENCES = 16
TOKENS = 2048
D = 512
FF = 2560
LAYERS = 2
NAMES = ("w_gate", "w_up", "w_down")
SHAPES = {"w_gate": (LAYERS, D, FF), "w_up": (LAYERS, D, FF), "w_down": (LAYERS, FF, D)}


def bump(key, n, height):
    away = (jnp.arange(n, dtype=jnp.int32) - jax.random.randint(key, (), 0, n, jnp.int32)) % n
    return jnp.where(away < n // 8, height, 1.0)


def together(key, own, strength):
    shared = jax.random.normal(key, own.shape[1:], jnp.float32)
    return (own + strength * shared) * lax.rsqrt(1 + strength * strength)


def setup_inputs(seed: int = 0, part: int = 0) -> dict:
    kx, kdy, ka, kb, kz, kf, kh, kl, *kw = jax.random.split(jax.random.key(seed), 8 + len(NAMES))
    kx, kdy, ka, kb = (jax.random.fold_in(k, part) for k in (kx, kdy, ka, kb))
    shape = (SEQUENCES, TOKENS, D)
    much_x, much_dy = jax.random.uniform(kz, (2,), jnp.float32, 0.0, 1.0)
    layers = 2.0 ** jax.random.uniform(kl, (LAYERS, 1, 1), jnp.float32, -1.0, 1.0)
    x = together(ka, jax.random.normal(kx, shape, jnp.float32), much_x) * bump(kf, D, 4.0)
    dy = together(kb, jax.random.normal(kdy, shape, jnp.float32), much_dy)
    drawn = {"x": x.astype(jnp.bfloat16), "dy": (dy * (SEQUENCES * TOKENS) ** -0.5).astype(jnp.bfloat16)}
    for key, name in zip(kw, NAMES, strict=True):
        w = jax.random.normal(key, SHAPES[name], jnp.float32) * SHAPES[name][1] ** -0.5
        drawn[name] = (w * {"w_gate": 1.0, "w_up": bump(kh, FF, 4.0), "w_down": layers}[name]).astype(jnp.bfloat16)
    return drawn


def matmul(a, w):
    return jnp.dot(a, w, preferred_element_type=jnp.float32).astype(jnp.bfloat16)


def normed(h):
    wide = h.astype(jnp.float32)
    scale = lax.rsqrt(jnp.mean(wide**2, -1, keepdims=True) + 1e-6)
    return (wide * scale).astype(jnp.bfloat16)


def layer(h, w):
    a = normed(h)
    gate = jnp.dot(a, w["w_gate"], preferred_element_type=jnp.float32)
    up = jnp.dot(a, w["w_up"], preferred_element_type=jnp.float32)
    return h + matmul((jax.nn.silu(gate) * up).astype(jnp.bfloat16), w["w_down"])


def stack(weights, h):
    return lax.scan(lambda h, w: (layer(h, w), None), h, weights)[0]


def reference(x, dy, w_gate, w_up, w_down):
    weights = dict(zip(NAMES, (w_gate, w_up, w_down), strict=True))

    def take(so_far, sequence):
        h, by_y = sequence
        _, back = jax.vjp(stack, weights, h)
        by_weights, by_h = back(by_y)
        return jax.tree.map(lambda total, term: total + term.astype(jnp.float32), so_far, by_weights), by_h

    none_yet = {name: jnp.zeros(w.shape, jnp.float32) for name, w in weights.items()}
    by_weights, by_x = lax.scan(take, none_yet, (x, dy))
    return (by_x, *(by_weights[name].astype(jnp.bfloat16) for name in NAMES))
```

```python
import functools
import math

import jax
import jax.numpy as jnp
from jax import lax
from jax.experimental import pallas as pl
from jax.experimental.pallas import tpu as pltpu
from jax.sharding import PartitionSpec as P

MESH = pl.DeviceIdType.MESH
F32, BF16 = jnp.float32, jnp.bfloat16
TILE = 512
DELAY = 2


def dot(a, b):
    return jnp.dot(a, b, preferred_element_type=F32)


def dot_t(a, b):
    return lax.dot_general(a, b, (((1,), (1,)), ((), ())), preferred_element_type=F32)


def rms_scale(wide):
    return lax.rsqrt(jnp.mean(wide * wide, -1, keepdims=True) + 1e-6)


def kernel(cfg, x_hbm, dy_hbm, wg_hbm, wu_hbm, wd_hbm, dx_hbm, g_hbm, u_hbm, d_hbm,
           WGU, WD, H, A, AT, DY, DYT, DGU, PJ, DWD, TK, SIB, SEND, RECV, OG, OU, OD,
           load_sem, ag_send, ag_recv, xy_send, xy_recv, sib_send, sib_recv,
           tk_send, tk_recv, msg_send, msg_recv, out_sem):
    n, side, xy, tokens, d, ff = cfg
    fb = d // 2
    half = ff // 2
    per_half = half // fb
    blocks = ff // fb
    rb = d // (2 * n)
    db = ff // (2 * n)
    kw = db // rb
    layer_slots = blocks + kw
    tickets = 2 * layer_slots
    far = n // 2
    ring = DELAY * far + 2
    tile = min(TILE, tokens // 4)
    tiles = tokens // tile
    tile_c = min(512, tokens // 4)
    tiles_c = tokens // tile_c

    me = lax.axis_index("dp")
    z, c = me // 2, me % 2
    rep = lax.axis_index("rep")
    right = {"dp": lax.rem(z + 1, n) * 2 + c}
    left = {"dp": lax.rem(z + n - 1, n) * 2 + c}
    partner = {"dp": z * 2 + 1 - c}
    gx, gy = rep // side, rep % side
    x_next = {"rep": (gx + 1 - 2 * (gx % 2)) * side + gy}
    y_next = {"rep": gx * side + gy + 1 - 2 * (gy % 2)}
    parity = (gx + gy) % 2

    def remote(src, dst, ss, rs, to):
        return pltpu.make_async_remote_copy(src_ref=src, dst_ref=dst, send_sem=ss, recv_sem=rs, device_id=to, device_id_type=MESH)

    def at(k):
        return lax.rem(z + k + 2 * n, n)

    AG = [(0, "gu", 0), (0, "gu", 1), (0, "wd", 0), (1, "wd", 0), (1, "gu", 0), (1, "gu", 1)]
    own_g = pl.ds(pl.multiple_of(me * rb, rb), rb)
    own_d = pl.ds(pl.multiple_of(me * db, rb), db)
    loads = []
    for t, (l, kind, h) in enumerate(AG):
        if kind == "gu":
            for m, w in enumerate((wg_hbm, wu_hbm)):
                loads.append((t, pltpu.make_async_copy(w.at[l, :, pl.ds(h * half, half)],
                                                       WGU.at[l, own_g, pl.ds((2 * h + m) * half, half)], load_sem.at[2 * t + m])))
        else:
            loads.append((t, pltpu.make_async_copy(wd_hbm.at[l], WD.at[l, own_d, :], load_sem.at[2 * t])))
    for _, copy in loads:
        copy.start()
    load_x = pltpu.make_async_copy(x_hbm.at[0], H, load_sem.at[2 * len(AG)])
    load_dy = pltpu.make_async_copy(dy_hbm.at[0], DY, load_sem.at[2 * len(AG) + 1])
    load_x.start()
    load_dy.start()

    barrier = pltpu.get_barrier_semaphore()
    friends = [left, right, partner] + ([x_next, y_next] if xy else [])
    for friend in friends:
        pl.semaphore_signal(barrier, inc=1, device_id=friend, device_id_type=MESH)
    pl.semaphore_wait(barrier, len(friends))

    share = 2 if xy else 1

    def piece(t, chip, part, cols):
        l, kind, h = AG[t]
        ref, rows, width, base = (WGU, rb, 2 * half, h * 2 * half) if kind == "gu" else (WD, db, d, 0)
        start = (2 * chip + c) * rows
        count = rows
        if part is not None:
            count = rows // 2
            start = start + part * count
        unit = math.gcd(rows, count)
        cw = width if cols is None else width // 2
        return ref.at[l, pl.ds(pl.multiple_of(start, math.gcd(unit, 16)), count), pl.ds(base + (cols or 0) * cw, cw)]

    def many(t, pieces, part, cols):
        l, kind, h = AG[t]
        ref, rows, width = (WGU, rb, 2 * half) if kind == "gu" else (WD, db, d)
        return ref.at[l, pl.ds(0, pieces * (rows // 2 if part else rows)), pl.ds(0, width // 2 if cols else width)]

    mine = parity if xy else None

    def hop(t, k, way):
        p = piece(t, at(-k if way == 0 else k), mine, way if k + 1 == n // 2 else None)
        return remote(p, p, ag_send.at[t, k, way], ag_recv.at[t, k, way], (right, left)[way])

    def arrive(t, k, way):
        p = piece(t, at(-(k + 1) if way == 0 else k + 1), mine, way if k + 1 == n // 2 else None)
        return remote(p, p, ag_send.at[t, k, way], ag_recv.at[t, k, way], (right, left)[way])

    def to_groups(t, chip):
        for m, friend in enumerate((x_next, y_next)):
            p = piece(t, chip, mine, m)
            remote(p, p, xy_send.at[t, m], xy_recv.at[t, m], friend).start()

    def group_wait(t, m):
        p = many(t, n - 1, True, True)
        return remote(p, p, xy_send.at[t, m], xy_recv.at[t, m], (x_next, y_next)[m])

    def partner_wait(t):
        p = many(t, n, None, None)
        return remote(p, p, sib_send.at[t], sib_recv.at[t], partner)

    def to_partner(t, chip, part):
        p = piece(t, chip, part, None)
        remote(p, p, sib_send.at[t], sib_recv.at[t], partner).start()

    def ag_step(t, k):
        if k == 0:
            for owner, copy in loads:
                if owner == t:
                    copy.wait()
            for way in (0, 1):
                hop(t, 0, way).start()
            to_partner(t, z, None)
        elif k <= n // 2:
            for way in (0, 1):
                arrive(t, k - 1, way).wait_recv()
                if k < n // 2:
                    hop(t, k, way).start()
            for chip in [at(-k), at(k)] if k < n // 2 else [at(k)]:
                if xy:
                    to_groups(t, chip)
                to_partner(t, chip, mine)
        elif k == n // 2 + 1 and xy:
            for m in (0, 1):
                group_wait(t, m).wait_recv()
            for b in range(1, n):
                to_partner(t, at(b), 1 - parity)

    last = n // 2 + 1
    rounds = len(AG) + last

    def ag_round(r):
        for t in range(len(AG)):
            if 0 <= r - t <= last:
                ag_step(t, r - t)

    def ready_round(t):
        return t + last

    for r in range(2):
        ag_round(r)
    load_x.wait()

    def turned(ref, ts, a):
        unit = (lax.broadcasted_iota(jnp.int32, (fb, fb), 0) == lax.broadcasted_iota(jnp.int32, (fb, fb), 1)).astype(F32).astype(BF16)
        for m in range(d // fb):
            ref[m * fb:(m + 1) * fb, ts] = dot_t(unit, a[:, m * fb:(m + 1) * fb]).astype(BF16)

    def normed_into(with_t):
        for i in range(tiles):
            ts = pl.ds(i * tile, tile)
            wide = H[ts, :].astype(F32)
            a = (wide * rms_scale(wide)).astype(BF16)
            A[ts, :] = a
            if with_t:
                turned(AT, ts, a)

    def transpose_dy():
        for i in range(tiles):
            ts = pl.ds(i * tile, tile)
            turned(DYT, ts, DY[ts, :])

    normed_into(False)
    load_dy.wait()
    transpose_dy()

    def columns(j):
        g = (j // per_half) * 2 * half + (j % per_half) * fb
        return pl.ds(pl.multiple_of(g, fb), fb), pl.ds(pl.multiple_of(g + half, fb), fb)

    def forward_block(j, _):
        gc, uc = columns(j)
        wg, wu = WGU[0, :, gc], WGU[0, :, uc]
        for i in range(tiles):
            ts = pl.ds(i * tile, tile)
            a = A[ts, :]
            g, u = dot(a, wg), dot(a, wu)
            s = 0.5 * jnp.tanh(0.5 * g) + 0.5
            DGU[ts, pl.ds(pl.multiple_of(j * fb, fb), fb)] = (g * s * u).astype(BF16)
        return 0

    for r in range(2, ready_round(0) + 1):
        ag_round(r)
    partner_wait(0).wait_recv()
    cut = (per_half + 1) // 2
    lax.fori_loop(0, cut, forward_block, 0)
    ag_round(ready_round(1))
    lax.fori_loop(cut, per_half, forward_block, 0)
    partner_wait(1).wait_recv()
    lax.fori_loop(per_half, per_half + cut, forward_block, 0)
    ag_round(ready_round(2))
    lax.fori_loop(per_half + cut, blocks, forward_block, 0)
    ag_round(ready_round(3))
    partner_wait(2).wait_recv()
    for i in range(tiles):
        ts = pl.ds(i * tile, tile)
        y = dot(DGU[ts, pl.ds(0, ff)], WD[0]).astype(BF16)
        H[ts, :] = H[ts, :] + y
        if i == 1:
            ag_round(ready_round(4))
    normed_into(True)
    for t in (3, 4):
        partner_wait(t).wait_recv()

    def slot_of(u):
        return lax.rem(u + 4 * ring, ring)

    def exchange(u):
        par = lax.rem(u, 2)
        return remote(TK.at[ring + par], SIB.at[slot_of(u)], tk_send.at[par], tk_recv.at[par], partner)

    def message(tau, way, lo):
        box = lax.rem(tau + 2 * DELAY, 2 * DELAY)
        return remote(SEND.at[way, box, pl.ds(lo, n - 1 - lo)], RECV.at[way, box, pl.ds(lo, n - 1 - lo)],
                      msg_send.at[way, box], msg_recv.at[way, box], (right, left)[way])

    def stage_of(tau):
        return max(0, -(-(tau - tickets) // DELAY)) if isinstance(tau, int) else 0

    def lowest(tau):
        return max(0, 2 * stage_of(tau) - 1)

    def ticket_row(u, q):
        keep, give = slot_of(u), ring + lax.rem(u + 2, 2)
        return keep + (give - keep) * ((q + c) % 2)

    def own_term(u, chip, part):
        cols = pl.ds(part * fb, fb)
        sl = slot_of(u)
        return TK[sl, chip, :, cols].astype(F32) + SIB[sl, chip, :, cols].astype(F32)

    def when(cond, f):
        if isinstance(cond, bool):
            if cond:
                f()
        else:
            pl.when(cond)(f)

    def spot(stage, way, part):
        return 0 if stage == 0 else 2 * stage - 1 + (part != way)

    def reduce_step(tau):
        static = isinstance(tau, int)
        box, came = lax.rem(tau + 2 * DELAY, 2 * DELAY), lax.rem(tau + DELAY, 2 * DELAY)
        sent = not static or stage_of(tau) < far

        def take():
            for way in (0, 1):
                message(tau - DELAY, way, lowest(tau - DELAY)).wait()

        def fresh():
            exchange(tau - 1).wait()

        if not static or stage_of(tau - DELAY) < far:
            when(tau >= 1 + DELAY, take)
        if not static or tau - 1 < tickets:
            when(tau >= 1, fresh)

        def work():
            for way in (0, 1):
                sign = 1 if way == 0 else -1
                for stage in range(stage_of(tau), far):
                    u, chip = tau - 1 - DELAY * stage, at(sign * (far - stage))
                    for part in (way, 1 - way) if stage else (way,):
                        total = own_term(u, chip, part)
                        if stage > 1 or (stage == 1 and part == way):
                            total += RECV[way, came, spot(stage - 1, way, part)].astype(F32)
                        SEND[way, box, spot(stage, way, part)] = total.astype(BF16)
            if sent:
                for way in (0, 1):
                    message(tau, way, lowest(tau)).start()

        def final():
            u = tau - 1 - DELAY * far
            total = [(RECV[0, came, spot(far - 1, 0, part)].astype(F32) + RECV[1, came, spot(far - 1, 1, part)].astype(F32)
                      + own_term(u, z, part)).astype(BF16) for part in (0, 1)]
            l, place = 1 - u // layer_slots, u % layer_slots

            def gate_up():
                cols = pl.ds(pl.multiple_of(place * fb, fb), fb)
                OG[l, :, cols] = total[0]
                OU[l, :, cols] = total[1]

            def down():
                rows = pl.ds(pl.multiple_of((place - blocks) * rb, rb), rb)
                for part in (0, 1):
                    OD[l, rows, pl.ds(part * fb, fb)] = total[part]

            when(place < blocks, gate_up)
            when(place >= blocks, down)

        when(tau >= 1 + DELAY * far, final)
        when(tau >= 1, work)

    def issue(tau):
        reduce_step(tau)
        when(tau >= 0, lambda: exchange(tau).start())

    def down_ticket(tau, k):
        for b in range(2 * n):
            TK[ticket_row(tau, b % 2), b // 2] = DWD[pl.ds(pl.multiple_of(b * db + k * rb, rb), rb), :]

    def gradients(j):
        tau_rows = pl.ds(pl.multiple_of(j * fb, fb), fb)
        before = lax.rem(j, blocks) if not isinstance(j, int) else j % blocks

        def part(m, tau):
            if m < 2:
                dw = dot(AT[...], DGU[:, columns(before)[m]]).astype(BF16)
                for b in range(2 * n):
                    TK[ticket_row(tau, b % 2), b // 2, :, pl.ds(m * fb, fb)] = dw[b * rb:(b + 1) * rb]
            else:
                DWD[tau_rows, :] = dot(DYT[...], PJ[...]).T.astype(BF16)

        return part

    def bw_layer(i, _):
        l = 1 - i
        base = i * layer_slots

        def block(j, _):
            tau = base + j - 1

            @pl.when((i == 0) & (j == 2))
            def _():
                ag_round(ready_round(5))

            @pl.when((i == 0) & (j == per_half))
            def _():
                partner_wait(5).wait_recv()

            gc, uc = columns(j)
            wg, wu = WGU[l, :, gc], WGU[l, :, uc]
            wd = WD[l, pl.ds(pl.multiple_of(j * fb, fb), fb), :]
            part = gradients(lax.rem(j + blocks, blocks + 1))
            part(2, tau)
            for q in range(tiles):
                ts = pl.ds(q * tile, tile)
                a = A[ts, :]
                dp = dot_t(DY[ts, :], wd).astype(BF16)
                g, u = dot(a, wg), dot(a, wu)
                if q < 2:
                    part(q, tau)
                dp = dp.astype(F32)
                s = 0.5 * jnp.tanh(0.5 * g) + 0.5
                gs = g * s
                PJ[ts, :] = (gs * u).astype(BF16)
                DGU[ts, uc] = (dp * gs).astype(BF16)
                DGU[ts, gc] = (dp * u * (s + gs * (1.0 - s))).astype(BF16)

            @pl.when(j == 0)
            def _():
                down_ticket(tau, kw - 1)

            issue(tau)
            return 0

        lax.fori_loop(0, blocks, block, 0)

        def tail_slot(k, _):
            tau = base + blocks - 1 + k

            @pl.when(k == 0)
            def _():
                part = gradients(blocks - 1)
                for m in range(3):
                    part(m, tau)

            @pl.when(k < tiles_c)
            def _():
                ts = pl.ds(pl.multiple_of(k * tile_c, tile_c), tile_c)
                da = dot_t(DGU[ts, :], WGU[l]).astype(BF16).astype(F32)
                wide = H[ts, :].astype(F32)
                scale = rms_scale(wide)
                dwide = da * scale - wide * (scale * scale * scale * jnp.mean(da * wide, -1, keepdims=True))
                DY[ts, :] = DY[ts, :] + dwide.astype(BF16)

            @pl.when((k == tiles_c) & (i == 0))
            def _():
                load_x.start()
                load_x.wait()
                normed_into(True)
                transpose_dy()

            @pl.when(k > 0)
            def _():
                down_ticket(tau, k - 1)

            issue(tau)
            return 0

        lax.fori_loop(0, kw, tail_slot, 0)
        return 0

    lax.fori_loop(0, 2, bw_layer, 0)

    out_x = pltpu.make_async_copy(DY, dx_hbm.at[0], out_sem.at[0])
    out_x.start()
    down_ticket(tickets - 1, kw - 1)
    for tau in range(tickets - 1, tickets + DELAY * far + 1):
        reduce_step(tau)
        if tau == tickets - 1:
            exchange(tau).start()
    outs = [pltpu.make_async_copy(a, b, out_sem.at[1 + m]) for m, (a, b) in enumerate(((OG, g_hbm), (OU, u_hbm), (OD, d_hbm)))]
    for copy in outs:
        copy.start()
    for t in range(len(AG)):
        for k in range(n // 2):
            for way in (0, 1):
                hop(t, k, way).wait_send()
        if xy:
            for m in (0, 1):
                group_wait(t, m).wait_send()
        partner_wait(t).wait_send()
    for copy in [out_x, *outs]:
        copy.wait()


def solution(mesh):
    groups = mesh.shape["rep"]
    n = mesh.shape["dp"] // 2
    side = math.isqrt(groups)
    xy = groups > 1

    def step(x, dy, w_gate, w_up, w_down):
        _, tokens, d = x.shape
        layers, _, ff = w_gate.shape
        rb = d // (2 * n)
        fb = d // 2
        ring = DELAY * (n // 2) + 2
        dma = pltpu.SemaphoreType.DMA
        call = pl.pallas_call(
            functools.partial(kernel, (n, side, xy, tokens, d, ff)),
            out_shape=(jax.ShapeDtypeStruct((1, tokens, d), BF16), jax.ShapeDtypeStruct((layers, rb, ff), BF16),
                       jax.ShapeDtypeStruct((layers, rb, ff), BF16), jax.ShapeDtypeStruct((layers, ff // (2 * n), d), BF16)),
            in_specs=[pl.BlockSpec(memory_space=pl.ANY)] * 5,
            out_specs=(pl.BlockSpec(memory_space=pl.ANY),) * 4,
            scratch_shapes=[
                pltpu.VMEM((layers, d, 2 * ff), BF16),
                pltpu.VMEM((layers, ff, d), BF16),
                pltpu.VMEM((tokens, d), BF16),
                pltpu.VMEM((tokens, d), BF16),
                pltpu.VMEM((d, tokens), BF16),
                pltpu.VMEM((tokens, d), BF16),
                pltpu.VMEM((d, tokens), BF16),
                pltpu.VMEM((tokens, 2 * ff), BF16),
                pltpu.VMEM((tokens, fb), BF16),
                pltpu.VMEM((ff + fb, d), BF16),
                pltpu.VMEM((ring + 2, n, rb, d), BF16),
                pltpu.VMEM((ring, n, rb, d), BF16),
                pltpu.VMEM((2, 2 * DELAY, n - 1, rb, fb), BF16),
                pltpu.VMEM((2, 2 * DELAY, n - 1, rb, fb), BF16),
                pltpu.VMEM((layers, rb, ff), BF16),
                pltpu.VMEM((layers, rb, ff), BF16),
                pltpu.VMEM((layers, ff // (2 * n), d), BF16),
                dma((14,)), dma((6, n // 2, 2)), dma((6, n // 2, 2)), dma((6, 2)), dma((6, 2)), dma((6,)), dma((6,)),
                dma((2,)), dma((2,)), dma((2, 2 * DELAY)), dma((2, 2 * DELAY)), dma((4,)),
            ],
            compiler_params=pltpu.CompilerParams(collective_id=0, has_side_effects=True, vmem_limit_bytes=67043328),
        )

        seqs, rows = P(("rep", "dp")), P(None, "dp")
        return jax.shard_map(call, mesh=mesh, in_specs=(seqs, seqs, rows, rows, rows),
                             out_specs=(seqs, P("rep", "dp"), P("rep", "dp"), P("rep", "dp")), check_vma=False)(x, dy, w_gate, w_up, w_down)

    return step
```

```python
import functools
import math

import jax
import jax.numpy as jnp
from jax import lax
from jax.experimental import pallas as pl
from jax.experimental.pallas import tpu as pltpu
from jax.sharding import PartitionSpec as P

MESH = pl.DeviceIdType.MESH
F32, BF16 = jnp.float32, jnp.bfloat16
TILE = 512
DELAY = 2


def dot(a, b):
    return jnp.dot(a, b, preferred_element_type=F32)


def dot_t(a, b):
    return lax.dot_general(a, b, (((1,), (1,)), ((), ())), preferred_element_type=F32)


def rms_scale(wide):
    return lax.rsqrt(jnp.mean(wide * wide, -1, keepdims=True) + 1e-6)


def kernel(cfg, x_hbm, dy_hbm, wg_hbm, wu_hbm, wd_hbm, dx_hbm, g_hbm, u_hbm, d_hbm,
           WGU, WD, H, A, AT, DY, DYT, DGU, PJ, DWD, TK, SIB, SEND, RECV, OG, OU, OD,
           load_sem, ag_send, ag_recv, xy_send, xy_recv, sib_send, sib_recv,
           tk_send, tk_recv, msg_send, msg_recv, out_sem):
    n, side, xy, tokens, d, ff = cfg
    fb = d // 2
    half = ff // 2
    per_half = half // fb
    blocks = ff // fb
    rb = d // (2 * n)
    db = ff // (2 * n)
    kw = db // rb
    layer_slots = blocks + kw
    tickets = 2 * layer_slots
    far = n // 2
    ring = DELAY * far + 2
    tile = min(TILE, tokens // 4)
    tiles = tokens // tile
    tile_c = min(512, tokens // 4)
    tiles_c = tokens // tile_c

    me = lax.axis_index("dp")
    z, c = me // 2, me % 2
    rep = lax.axis_index("rep")
    right = {"dp": lax.rem(z + 1, n) * 2 + c}
    left = {"dp": lax.rem(z + n - 1, n) * 2 + c}
    partner = {"dp": z * 2 + 1 - c}
    gx, gy = rep // side, rep % side
    x_next = {"rep": (gx + 1 - 2 * (gx % 2)) * side + gy}
    y_next = {"rep": gx * side + gy + 1 - 2 * (gy % 2)}
    parity = (gx + gy) % 2

    def remote(src, dst, ss, rs, to):
        return pltpu.make_async_remote_copy(src_ref=src, dst_ref=dst, send_sem=ss, recv_sem=rs, device_id=to, device_id_type=MESH)

    def at(k):
        return lax.rem(z + k + 2 * n, n)

    AG = [(0, "gu", 0), (0, "gu", 1), (0, "wd", 0), (1, "wd", 0), (1, "gu", 0), (1, "gu", 1)]
    own_g = pl.ds(pl.multiple_of(me * rb, rb), rb)
    own_d = pl.ds(pl.multiple_of(me * db, rb), db)
    loads = []
    for t, (l, kind, h) in enumerate(AG):
        if kind == "gu":
            for m, w in enumerate((wg_hbm, wu_hbm)):
                loads.append((t, pltpu.make_async_copy(w.at[l, :, pl.ds(h * half, half)],
                                                       WGU.at[l, own_g, pl.ds((2 * h + m) * half, half)], load_sem.at[2 * t + m])))
        else:
            loads.append((t, pltpu.make_async_copy(wd_hbm.at[l], WD.at[l, own_d, :], load_sem.at[2 * t])))
    for _, copy in loads:
        copy.start()
    load_x = pltpu.make_async_copy(x_hbm.at[0], H, load_sem.at[2 * len(AG)])
    load_dy = pltpu.make_async_copy(dy_hbm.at[0], DY, load_sem.at[2 * len(AG) + 1])
    load_x.start()
    load_dy.start()

    barrier = pltpu.get_barrier_semaphore()
    friends = [left, right, partner] + ([x_next, y_next] if xy else [])
    for friend in friends:
        pl.semaphore_signal(barrier, inc=1, device_id=friend, device_id_type=MESH)
    pl.semaphore_wait(barrier, len(friends))

    share = 2 if xy else 1

    def piece(t, chip, part, cols):
        l, kind, h = AG[t]
        ref, rows, width, base = (WGU, rb, 2 * half, h * 2 * half) if kind == "gu" else (WD, db, d, 0)
        start = (2 * chip + c) * rows
        count = rows
        if part is not None:
            count = rows // 2
            start = start + part * count
        unit = math.gcd(rows, count)
        cw = width if cols is None else width // 2
        return ref.at[l, pl.ds(pl.multiple_of(start, math.gcd(unit, 16)), count), pl.ds(base + (cols or 0) * cw, cw)]

    def many(t, pieces, part, cols):
        l, kind, h = AG[t]
        ref, rows, width = (WGU, rb, 2 * half) if kind == "gu" else (WD, db, d)
        return ref.at[l, pl.ds(0, pieces * (rows // 2 if part else rows)), pl.ds(0, width // 2 if cols else width)]

    mine = parity if xy else None

    def hop(t, k, way):
        p = piece(t, at(-k if way == 0 else k), mine, way if k + 1 == n // 2 else None)
        return remote(p, p, ag_send.at[t, k, way], ag_recv.at[t, k, way], (right, left)[way])

    def arrive(t, k, way):
        p = piece(t, at(-(k + 1) if way == 0 else k + 1), mine, way if k + 1 == n // 2 else None)
        return remote(p, p, ag_send.at[t, k, way], ag_recv.at[t, k, way], (right, left)[way])

    def to_groups(t, chip):
        for m, friend in enumerate((x_next, y_next)):
            p = piece(t, chip, mine, m)
            remote(p, p, xy_send.at[t, m], xy_recv.at[t, m], friend).start()

    def group_wait(t, m):
        p = many(t, n - 1, True, True)
        return remote(p, p, xy_send.at[t, m], xy_recv.at[t, m], (x_next, y_next)[m])

    def partner_wait(t):
        p = many(t, n, None, None)
        return remote(p, p, sib_send.at[t], sib_recv.at[t], partner)

    def to_partner(t, chip, part):
        p = piece(t, chip, part, None)
        remote(p, p, sib_send.at[t], sib_recv.at[t], partner).start()

    def ag_step(t, k):
        if k == 0:
            for owner, copy in loads:
                if owner == t:
                    copy.wait()
            for way in (0, 1):
                hop(t, 0, way).start()
            to_partner(t, z, None)
        elif k <= n // 2:
            for way in (0, 1):
                arrive(t, k - 1, way).wait_recv()
                if k < n // 2:
                    hop(t, k, way).start()
            for chip in [at(-k), at(k)] if k < n // 2 else [at(k)]:
                if xy:
                    to_groups(t, chip)
                to_partner(t, chip, mine)
        elif k == n // 2 + 1 and xy:
            for m in (0, 1):
                group_wait(t, m).wait_recv()
            for b in range(1, n):
                to_partner(t, at(b), 1 - parity)

    last = n // 2 + 1
    rounds = len(AG) + last

    def ag_round(r):
        for t in range(len(AG)):
            if t == 0 and r == 0:
                ag_step(0, 0)
            elif 1 <= r - t <= last:
                ag_step(t, r - t)
            elif t == r + 1:
                ag_step(t, 0)

    def ready_round(t):
        return t + last

    for r in range(2):
        ag_round(r)
    load_x.wait()

    def turned(ref, ts, a):
        unit = (lax.broadcasted_iota(jnp.int32, (fb, fb), 0) == lax.broadcasted_iota(jnp.int32, (fb, fb), 1)).astype(F32).astype(BF16)
        for m in range(d // fb):
            ref[m * fb:(m + 1) * fb, ts] = dot_t(unit, a[:, m * fb:(m + 1) * fb]).astype(BF16)

    def normed_into(with_t):
        for i in range(tiles):
            ts = pl.ds(i * tile, tile)
            wide = H[ts, :].astype(F32)
            a = (wide * rms_scale(wide)).astype(BF16)
            A[ts, :] = a
            if with_t:
                turned(AT, ts, a)

    def transpose_dy():
        for i in range(tiles):
            ts = pl.ds(i * tile, tile)
            turned(DYT, ts, DY[ts, :])

    normed_into(False)
    load_dy.wait()
    transpose_dy()

    def columns(j):
        g = (j // per_half) * 2 * half + (j % per_half) * fb
        return pl.ds(pl.multiple_of(g, fb), fb), pl.ds(pl.multiple_of(g + half, fb), fb)

    def forward_block(j, _):
        gc, uc = columns(j)
        wg, wu = WGU[0, :, gc], WGU[0, :, uc]
        for i in range(tiles):
            ts = pl.ds(i * tile, tile)
            a = A[ts, :]
            g, u = dot(a, wg), dot(a, wu)
            s = 0.5 * jnp.tanh(0.5 * g) + 0.5
            DGU[ts, pl.ds(pl.multiple_of(j * fb, fb), fb)] = (g * s * u).astype(BF16)
        return 0

    for r in range(2, ready_round(0) + 1):
        ag_round(r)
    partner_wait(0).wait_recv()
    cut = (per_half + 1) // 2
    lax.fori_loop(0, cut, forward_block, 0)
    ag_round(ready_round(1))
    lax.fori_loop(cut, per_half, forward_block, 0)
    partner_wait(1).wait_recv()
    lax.fori_loop(per_half, per_half + cut, forward_block, 0)
    ag_round(ready_round(2))
    lax.fori_loop(per_half + cut, blocks, forward_block, 0)
    ag_round(ready_round(3))
    partner_wait(2).wait_recv()
    for i in range(tiles):
        ts = pl.ds(i * tile, tile)
        y = dot(DGU[ts, pl.ds(0, ff)], WD[0]).astype(BF16)
        H[ts, :] = H[ts, :] + y
        if i == 1:
            ag_round(ready_round(4))
    normed_into(True)
    for t in (3, 4):
        partner_wait(t).wait_recv()

    def slot_of(u):
        return lax.rem(u + 4 * ring, ring)

    def exchange(u):
        par = lax.rem(u + 2, 2)
        return remote(TK.at[ring + par], SIB.at[slot_of(u)], tk_send.at[par], tk_recv.at[par], partner)

    def message(tau, way, lo):
        box = lax.rem(tau + 2 * DELAY, 2 * DELAY)
        return remote(SEND.at[way, box, pl.ds(lo, n - 1 - lo)], RECV.at[way, box, pl.ds(lo, n - 1 - lo)],
                      msg_send.at[way, box], msg_recv.at[way, box], (right, left)[way])

    def stage_of(tau):
        return max(0, -(-(tau - tickets) // DELAY)) if isinstance(tau, int) else 0

    def lowest(tau):
        return max(0, 2 * stage_of(tau) - 1)

    def ticket_row(u, q):
        keep, give = slot_of(u), ring + lax.rem(u + 2, 2)
        return keep + (give - keep) * ((q + c) % 2)

    def own_term(u, chip, part):
        cols = pl.ds(part * fb, fb)
        sl = slot_of(u)
        return TK[sl, chip, :, cols].astype(F32) + SIB[sl, chip, :, cols].astype(F32)

    def when(cond, f):
        if isinstance(cond, bool):
            if cond:
                f()
        else:
            pl.when(cond)(f)

    def spot(stage, way, part):
        return 0 if stage == 0 else 2 * stage - 1 + (part != way)

    def came_in(tau):
        return lax.rem(tau + DELAY, 2 * DELAY)

    def collect(tau):
        static = isinstance(tau, int)
        came = came_in(tau)

        def take():
            for way in (0, 1):
                message(tau - DELAY, way, lowest(tau - DELAY)).wait()

        def fresh():
            exchange(tau - 1).wait()

        def final():
            u = tau - 1 - DELAY * far
            total = [(RECV[0, came, spot(far - 1, 0, part)].astype(F32) + RECV[1, came, spot(far - 1, 1, part)].astype(F32)
                      + own_term(u, z, part)).astype(BF16) for part in (0, 1)]
            l, place = 1 - u // layer_slots, u % layer_slots

            def gate_up():
                cols = pl.ds(pl.multiple_of(place * fb, fb), fb)
                OG[l, :, cols] = total[0]
                OU[l, :, cols] = total[1]

            def down():
                rows = pl.ds(pl.multiple_of((place - blocks) * rb, rb), rb)
                for part in (0, 1):
                    OD[l, rows, pl.ds(part * fb, fb)] = total[part]

            when(place < blocks, gate_up)
            when(place >= blocks, down)

        if not static or stage_of(tau - DELAY) < far:
            when(tau >= DELAY - 1, take)
        if not static or tau - 1 < tickets:
            when(tau >= 0, fresh)
        when(tau >= 1 + DELAY * far, final)

    def combine(tau):
        box = lax.rem(tau + 2 * DELAY, 2 * DELAY)
        for way in (0, 1):
            sign = 1 if way == 0 else -1
            for stage in range(stage_of(tau), far):
                u, chip = tau - 1 - DELAY * stage, at(sign * (far - stage))
                for part in (way, 1 - way) if stage else (way,):
                    total = own_term(u, chip, part)
                    if stage > 1 or (stage == 1 and part == way):
                        total += RECV[way, came_in(tau), spot(stage - 1, way, part)].astype(F32)
                    SEND[way, box, spot(stage, way, part)] = total.astype(BF16)

    def send(tau):
        if stage_of(tau) < far:
            for way in (0, 1):
                message(tau, way, lowest(tau)).start()

    def issue(tau):
        send(tau)
        exchange(tau).start()

    def down_ticket(tau, k):
        for b in range(2 * n):
            TK[ticket_row(tau, b % 2), b // 2] = DWD[pl.ds(pl.multiple_of(b * db + k * rb, rb), rb), :]

    def gradients(j):
        tau_rows = pl.ds(pl.multiple_of(j * fb, fb), fb)
        before = lax.rem(j, blocks) if not isinstance(j, int) else j % blocks

        def part(m, tau):
            if m < 2:
                dw = dot(AT[...], DGU[:, columns(before)[m]]).astype(BF16)
                for b in range(2 * n):
                    TK[ticket_row(tau, b % 2), b // 2, :, pl.ds(m * fb, fb)] = dw[b * rb:(b + 1) * rb]
            else:
                DWD[tau_rows, :] = dot(DYT[...], PJ[...]).T.astype(BF16)

        return part

    def bw_layer(i, _):
        l = 1 - i
        base = i * layer_slots

        def block(j, _):
            tau = base + j - 1

            @pl.when((i == 0) & (j == 2))
            def _():
                ag_round(ready_round(5))

            @pl.when((i == 0) & (j == per_half))
            def _():
                partner_wait(5).wait_recv()

            gc, uc = columns(j)
            wg, wu = WGU[l, :, gc], WGU[l, :, uc]
            wd = WD[l, pl.ds(pl.multiple_of(j * fb, fb), fb), :]
            part = gradients(lax.rem(j + blocks, blocks + 1))
            part(2, tau)
            for q in range(tiles):
                ts = pl.ds(q * tile, tile)
                a = A[ts, :]
                dp = dot_t(DY[ts, :], wd).astype(BF16)
                g, u = dot(a, wg), dot(a, wu)
                if q % 2 == 0:
                    part(q // 2, tau)
                dp = dp.astype(F32)
                s = 0.5 * jnp.tanh(0.5 * g) + 0.5
                gs = g * s
                PJ[ts, :] = (gs * u).astype(BF16)
                DGU[ts, uc] = (dp * gs).astype(BF16)
                DGU[ts, gc] = (dp * u * (s + gs * (1.0 - s))).astype(BF16)

            @pl.when(j == 0)
            def _():
                down_ticket(tau, kw - 1)

            collect(tau)
            combine(tau)
            issue(tau)
            return 0

        lax.fori_loop(0, blocks, block, 0)

        def tail_slot(k, _):
            tau = base + blocks - 1 + k

            @pl.when(k == 0)
            def _():
                part = gradients(blocks - 1)
                for m in range(3):
                    part(m, tau)

            @pl.when(k < tiles_c)
            def _():
                ts = pl.ds(pl.multiple_of(k * tile_c, tile_c), tile_c)
                da = dot_t(DGU[ts, :], WGU[l]).astype(BF16).astype(F32)
                wide = H[ts, :].astype(F32)
                scale = rms_scale(wide)
                dwide = da * scale - wide * (scale * scale * scale * jnp.mean(da * wide, -1, keepdims=True))
                DY[ts, :] = DY[ts, :] + dwide.astype(BF16)

            @pl.when((k == tiles_c) & (i == 0))
            def _():
                load_x.start()
                load_x.wait()
                normed_into(True)
                transpose_dy()

            @pl.when(k > 0)
            def _():
                down_ticket(tau, k - 1)

            collect(tau)
            combine(tau)
            issue(tau)
            return 0

        lax.fori_loop(0, kw, tail_slot, 0)
        return 0

    lax.fori_loop(0, 2, bw_layer, 0)

    out_x = pltpu.make_async_copy(DY, dx_hbm.at[0], out_sem.at[0])
    out_x.start()
    down_ticket(tickets - 1, kw - 1)
    for tau in range(tickets - 1, tickets + DELAY * far + 1):
        collect(tau)
        combine(tau)
        send(tau)
        if tau == tickets - 1:
            exchange(tau).start()
    outs = [pltpu.make_async_copy(a, b, out_sem.at[1 + m]) for m, (a, b) in enumerate(((OG, g_hbm), (OU, u_hbm), (OD, d_hbm)))]
    for copy in outs:
        copy.start()
    for t in range(len(AG)):
        for k in range(n // 2):
            for way in (0, 1):
                hop(t, k, way).wait_send()
        if xy:
            for m in (0, 1):
                group_wait(t, m).wait_send()
        partner_wait(t).wait_send()
    for copy in [out_x, *outs]:
        copy.wait()


def solution(mesh):
    groups = mesh.shape["rep"]
    n = mesh.shape["dp"] // 2
    side = math.isqrt(groups)
    xy = groups > 1

    def step(x, dy, w_gate, w_up, w_down):
        _, tokens, d = x.shape
        layers, _, ff = w_gate.shape
        rb = d // (2 * n)
        fb = d // 2
        ring = DELAY * (n // 2) + 2
        dma = pltpu.SemaphoreType.DMA
        call = pl.pallas_call(
            functools.partial(kernel, (n, side, xy, tokens, d, ff)),
            out_shape=(jax.ShapeDtypeStruct((1, tokens, d), BF16), jax.ShapeDtypeStruct((layers, rb, ff), BF16),
                       jax.ShapeDtypeStruct((layers, rb, ff), BF16), jax.ShapeDtypeStruct((layers, ff // (2 * n), d), BF16)),
            in_specs=[pl.BlockSpec(memory_space=pl.ANY)] * 5,
            out_specs=(pl.BlockSpec(memory_space=pl.ANY),) * 4,
            scratch_shapes=[
                pltpu.VMEM((layers, d, 2 * ff), BF16),
                pltpu.VMEM((layers, ff, d), BF16),
                pltpu.VMEM((tokens, d), BF16),
                pltpu.VMEM((tokens, d), BF16),
                pltpu.VMEM((d, tokens), BF16),
                pltpu.VMEM((tokens, d), BF16),
                pltpu.VMEM((d, tokens), BF16),
                pltpu.VMEM((tokens, 2 * ff), BF16),
                pltpu.VMEM((tokens, fb), BF16),
                pltpu.VMEM((ff + fb, d), BF16),
                pltpu.VMEM((ring + 2, n, rb, d), BF16),
                pltpu.VMEM((ring, n, rb, d), BF16),
                pltpu.VMEM((2, 2 * DELAY, n - 1, rb, fb), BF16),
                pltpu.VMEM((2, 2 * DELAY, n - 1, rb, fb), BF16),
                pltpu.VMEM((layers, rb, ff), BF16),
                pltpu.VMEM((layers, rb, ff), BF16),
                pltpu.VMEM((layers, ff // (2 * n), d), BF16),
                dma((14,)), dma((6, n // 2, 2)), dma((6, n // 2, 2)), dma((6, 2)), dma((6, 2)), dma((6,)), dma((6,)),
                dma((2,)), dma((2,)), dma((2, 2 * DELAY)), dma((2, 2 * DELAY)), dma((4,)),
            ],
            compiler_params=pltpu.CompilerParams(collective_id=0, has_side_effects=True, vmem_limit_bytes=67043328),
        )

        seqs, rows = P(("rep", "dp")), P(None, "dp")
        return jax.shard_map(call, mesh=mesh, in_specs=(seqs, seqs, rows, rows, rows),
                             out_specs=(seqs, P("rep", "dp"), P("rep", "dp"), P("rep", "dp")), check_vma=False)(x, dy, w_gate, w_up, w_down)

    return step
```
